32 devices in a mesh: aa: 2 (over y), ba: 4 (over z), col: 4 (over x, core).
Axes of the slice: x: 2, y: 2, z: 4, core: 2. Of those that a mesh axis runs over, the one named last changes fastest.
Arguments:
- amplitudes: bfloat16 [384, 384, 384], P('aa', 'ba', 'col'), as said below
- factors: bfloat16 [4, 384, 384], replicated, may hold values from -0.15625 to 0.15625
- energies: float32 [384], replicated, may hold values from 0.3 to 1.5
Outputs:
- sigma: bfloat16 [384, 384, 384], P('aa', 'ba', 'col')
The draws below stay inside these ranges and needn't reach their ends.
Inputs may be any that keep to these rules, and one draw needn't show every extreme that they name: amplitudes is antisymmetric: exchanging any two of its three indices changes its sign.
All inputs are finite; a program needn't handle non-finite values.
Results may differ from the reference program's by a relative error of at most 0.0065.
Values may be sent and summed in bfloat16 or wider, within the bound.
A program may use at most 320 MiB of HBM per device.

```python
import jax
import jax.numpy as jnp
from jax import lax

V = 384
NAUX = 4


def draw_amplitudes(key, part):
    source = jax.random.normal(key, (V, V, V), jnp.float32)
    even = source + jnp.transpose(source, (1, 2, 0)) + jnp.transpose(source, (2, 0, 1))
    odd_part = jnp.transpose(source, (1, 0, 2)) + jnp.transpose(source, (0, 2, 1)) + jnp.transpose(source, (2, 1, 0))
    return ((even - odd_part) / 2.449489742783178).astype(jnp.bfloat16)


def centred(key, dims, deviation, most, held_as=jnp.bfloat16):
    array = jax.random.normal(key, dims, jnp.float32) * deviation
    return jnp.minimum(jnp.maximum(array, -most), most).astype(held_as)


def setup_inputs(seed: int = 0) -> dict:
    key_list = jax.random.split(jax.random.key(seed), 4)
    return {
        "amplitudes": draw_amplitudes(jax.random.fold_in(key_list[3], 71), 0),
        "factors": centred(key_list[1], (NAUX, V, V), (4 * V) ** -0.5, 0.15625),
        "energies": jnp.clip(jax.random.uniform(key_list[2], (V,), jnp.float32, 0.3, 1.5), 0.3, 1.5),
    }


def reference(amplitudes, factors, energies):
    amps = amplitudes.astype(jnp.float32)

    def step(running, matrix):
        factor = matrix.astype(jnp.float32)
        along_a = jnp.einsum("ae,ebc->abc", factor, amps)
        along_b = jnp.einsum("be,aec->abc", factor, amps)
        along_a = lax.optimization_barrier(along_a.astype(jnp.bfloat16)).astype(jnp.float32)
        along_b = lax.optimization_barrier(along_b.astype(jnp.bfloat16)).astype(jnp.float32)
        ladder_ab = jnp.einsum("afc,bf->abc", along_a, factor)
        ladder_ac = jnp.einsum("abf,cf->abc", along_a, factor)
        ladder_bc = jnp.einsum("abf,cf->abc", along_b, factor)
        return running + ladder_ab + ladder_bc + ladder_ac, None

    start_sum = jnp.zeros((V, V, V), jnp.float32)
    total_sum, unused = lax.scan(step, start_sum, factors)
    shifts = energies[:, None, None] + energies[None, :, None] + energies[None, None, :]
    return (2.0 * total_sum + shifts * amps).astype(jnp.bfloat16)
```

```python
import functools

import jax
import jax.numpy as jnp
from jax import lax
from jax.experimental import pallas as pl
from jax.experimental.pallas import tpu as pltpu
from jax.sharding import PartitionSpec as P


def on_device(amplitudes, factors, energies):
    width_a, width_b, width_c = amplitudes.shape
    fitting = factors.shape[0]
    merged = width_b * width_c
    index_a = lax.axis_index("aa")
    index_b = lax.axis_index("ba")
    index_c = lax.axis_index("col")
    rows_a = lax.dynamic_slice_in_dim(factors, index_a * width_a, width_a, 1)
    rows_b = lax.dynamic_slice_in_dim(factors, index_b * width_b, width_b, 1)
    rows_c = lax.dynamic_slice_in_dim(factors, index_c * width_c, width_c, 1)
    energy_a = lax.dynamic_slice_in_dim(energies, index_a * width_a, width_a, 0)
    energy_b = lax.dynamic_slice_in_dim(energies, index_b * width_b, width_b, 0)
    energy_c = lax.dynamic_slice_in_dim(energies, index_c * width_c, width_c, 0)

    def close_c(portion):
        term = jnp.einsum("pabf,pcf->abc", portion, rows_c, preferred_element_type=jnp.float32)
        return term.reshape(width_a, merged)

    shape_x = (fitting, width_a, width_b, width_c)
    shape_w = (width_a, width_b, width_c)
    columns = rows_a
    term = jnp.einsum(
        "pae,ebc->pabc",
        columns,
        lax.all_gather(amplitudes, "aa", axis=0, tiled=True),
        preferred_element_type=jnp.float32,
    )
    along_a = term.reshape(fitting, width_a, merged).astype(jnp.bfloat16).reshape(shape_x)
    columns = rows_b
    term = jnp.einsum(
        "pbe,aec->pabc",
        columns,
        lax.all_gather(amplitudes, "ba", axis=1, tiled=True),
        preferred_element_type=jnp.float32,
    )
    along_b = term.reshape(fitting, width_a, merged).astype(jnp.bfloat16).reshape(shape_x)
    ladder_ac = close_c(lax.all_gather(along_a, "col", axis=3, tiled=True))
    ladder_bc = close_c(lax.all_gather(along_b, "col", axis=3, tiled=True))
    block_b = lax.dynamic_slice_in_dim(factors, index_b * width_b, width_b, 2)
    terms_ab = jnp.einsum("pafc,pbf->abc", along_a, block_b, preferred_element_type=jnp.float32)
    ladder_ab = (
        lax.psum_scatter(terms_ab.astype(jnp.bfloat16), "ba", scatter_dimension=1, tiled=True)
        .astype(jnp.float32)
        .reshape(width_a, merged)
    )
    shifts = energy_a[:, None, None] + energy_b[None, :, None] + energy_c[None, None, :]
    ladders = (ladder_ab + ladder_bc + ladder_ac).reshape(shape_w)
    result = 2.0 * ladders + shifts * amplitudes.astype(jnp.float32)
    return result.astype(jnp.bfloat16)


LANES = 128


def pack_kernel(rows, amplitudes_ref, out_ref, wide):
    width_a, group, width_c = amplitudes_ref.shape
    wide[:, :width_c] = amplitudes_ref[...].astype(jnp.float32).reshape(width_a * group, width_c)
    for b in range(group):
        block = wide[pl.ds(b, width_a, stride=group), :][:, :width_c]
        out_ref[b] = folded(block, rows).astype(out_ref.dtype)


def folded(block, rows):
    width_a, width_c = block.shape
    spare = LANES - width_c
    rest = block[rows:]
    extra = jnp.concatenate([rest[:, i * spare : (i + 1) * spare] for i in range(width_c // spare)], axis=0)
    return jnp.concatenate([block[:rows], extra], axis=1)


def unfolded(packed, width_a, width_c):
    rows = packed.shape[0]
    spare = LANES - width_c
    left = width_a - rows
    rest = [packed[i * left : (i + 1) * left, width_c:] for i in range(width_c // spare)]
    return jnp.concatenate([packed[:, :width_c], jnp.concatenate(rest, axis=1)], axis=0)


def pack(amplitudes, group, rows):
    width_a, width_b, width_c = amplitudes.shape
    return pl.pallas_call(
        functools.partial(pack_kernel, rows),
        grid=(width_b // group,),
        in_specs=[pl.BlockSpec((width_a, group, width_c), lambda g: (0, g, 0))],
        out_specs=pl.BlockSpec((group, rows, LANES), lambda g: (g, 0, 0)),
        out_shape=jax.ShapeDtypeStruct((width_b, rows, LANES), amplitudes.dtype),
        scratch_shapes=[pltpu.VMEM((width_a * group, LANES), jnp.float32)],
    )(amplitudes)


def ladder_kernel(sizes, portion_ref, stacked_ref, closing_ref, ladder_ref, rows_ref, slab, once, wide):
    n_a, n_c, width_a, width_c, share = sizes
    count = portion_ref.shape[1]
    size = stacked_ref.shape[1]
    fitting = stacked_ref.shape[0] // size
    for s in range(count):
        for i in range(n_a):
            for k in range(n_c):
                block = unfolded(portion_ref[i * n_c + k, s].astype(jnp.float32), width_a, width_c)
                wide[i * width_a : (i + 1) * width_a, k * width_c : (k + 1) * width_c] = block
        slab[:, s * size : (s + 1) * size] = wide[...].astype(slab.dtype)
    for p in range(fitting):
        half = jnp.dot(
            stacked_ref[p * size : (p + 1) * size, :], slab[...], preferred_element_type=jnp.float32
        ).astype(once.dtype)
        for s in range(count):
            once[s * size : (s + 1) * size, p * size : (p + 1) * size] = half[:, s * size : (s + 1) * size]
    for s in range(count):
        wide[...] = jnp.dot(
            once[s * size : (s + 1) * size, :], closing_ref[...], preferred_element_type=jnp.float32
        )
        ladder_ref[s] = wide[...].astype(ladder_ref.dtype)
        for d in range(size // share):
            rows_ref[d, s * share : (s + 1) * share, :] = wide[d * share : (d + 1) * share, :].astype(rows_ref.dtype)


def ladders_of_slabs(sizes, portion, stacked, closing, count):
    n_a, n_c, width_a, width_c, share = sizes
    peers, _, rows, _ = portion.shape
    size = stacked.shape[1]
    devices = size // share
    fitting = stacked.shape[0] // size
    return pl.pallas_call(
        functools.partial(ladder_kernel, sizes),
        grid=(share // count,),
        in_specs=[
            pl.BlockSpec((peers, count, rows, LANES), lambda g: (0, g, 0, 0)),
            pl.BlockSpec(stacked.shape, lambda g: (0, 0)),
            pl.BlockSpec(closing.shape, lambda g: (0, 0)),
        ],
        out_specs=[
            pl.BlockSpec((count, size, size), lambda g: (g, 0, 0)),
            pl.BlockSpec((devices, count * share, size), lambda g: (0, g, 0)),
        ],
        out_shape=[
            jax.ShapeDtypeStruct((share, size, size), portion.dtype),
            jax.ShapeDtypeStruct((devices, share * share, size), portion.dtype),
        ],
        scratch_shapes=[
            pltpu.VMEM((size, count * size), portion.dtype),
            pltpu.VMEM((count * size, fitting * size), portion.dtype),
            pltpu.VMEM((size, size), jnp.float32),
        ],
        cost_estimate=pl.CostEstimate(
            flops=4 * share * fitting * size**3, bytes_accessed=8 * share * size * size, transcendentals=0
        ),
    )(portion, stacked, closing)


def joining_kernel(sizes, ladder_ref, rows_ref, out_ref, wide):
    n_a, n_b, n_c, width_a, width_c, rows = sizes
    share, size, _ = ladder_ref.shape
    chunk = share * share

    @pl.when(pl.program_id(0) == 0)
    def _():
        for j in range(n_b):
            for i in range(n_a):
                for k in range(n_c):
                    at = ((j * n_a + i) * n_c + k) * chunk
                    piece = rows_ref[(i * n_b + j) * n_c + k].astype(jnp.float32)
                    for tile in range(size // LANES):
                        wide[tile, at : at + chunk, :] = piece[:, tile * LANES : (tile + 1) * LANES]

    for b in range(share):
        tiles = [wide[tile, pl.ds(b, size, stride=share), :] for tile in range(size // LANES)]
        crossed = jnp.concatenate(tiles, axis=1)
        total = ladder_ref[b].astype(jnp.float32) + crossed.T - crossed
        for i in range(n_a):
            for k in range(n_c):
                block = total[i * width_a : (i + 1) * width_a, k * width_c : (k + 1) * width_c]
                out_ref[i * n_c + k, b] = folded(block, rows).astype(out_ref.dtype)


def joined(sizes, ladder, crossing):
    n_a, n_b, n_c, width_a, width_c, rows = sizes
    share, size, _ = ladder.shape
    return pl.pallas_call(
        functools.partial(joining_kernel, sizes),
        grid=(1,),
        in_specs=[
            pl.BlockSpec(ladder.shape, lambda g: (0, 0, 0)),
            pl.BlockSpec(crossing.shape, lambda g: (0, 0, 0)),
        ],
        out_specs=pl.BlockSpec((n_a * n_c, share, rows, LANES), lambda g: (0, 0, 0, 0)),
        out_shape=jax.ShapeDtypeStruct((n_a * n_c, share, rows, LANES), ladder.dtype),
        scratch_shapes=[pltpu.VMEM((size // LANES, size * share, LANES), jnp.float32)],
    )(ladder, crossing)


def closing_kernel(total_ref, amplitudes_ref, shift_a_ref, shift_b_ref, shift_c_ref, out_ref, wide):
    width_a, group, width_c = amplitudes_ref.shape
    for b in range(group):
        block = unfolded(total_ref[b].astype(jnp.float32), width_a, width_c)
        block = jnp.concatenate([block, jnp.zeros((width_a, LANES - width_c), jnp.float32)], axis=1)
        wide[pl.ds(b, width_a, stride=group), :] = block
    shifts = shift_a_ref[...] + shift_b_ref[...] + shift_c_ref[...]
    total = wide[:, :width_c].reshape(width_a, group, width_c)
    out_ref[...] = (2.0 * total + shifts * amplitudes_ref[...].astype(jnp.float32)).astype(out_ref.dtype)


def closed(total, amplitudes, energy_a, energy_b, energy_c, group):
    width_a, width_b, width_c = amplitudes.shape
    rows = total.shape[1]
    block = pl.BlockSpec((width_a, group, width_c), lambda g: (0, g, 0))
    return pl.pallas_call(
        closing_kernel,
        grid=(width_b // group,),
        in_specs=[
            pl.BlockSpec((group, rows, LANES), lambda g: (g, 0, 0)),
            block,
            pl.BlockSpec((width_a, 1, 1), lambda g: (0, 0, 0)),
            pl.BlockSpec((1, group, 1), lambda g: (0, g, 0)),
            pl.BlockSpec((1, 1, width_c), lambda g: (0, 0, 0)),
        ],
        out_specs=block,
        out_shape=jax.ShapeDtypeStruct(amplitudes.shape, amplitudes.dtype),
        scratch_shapes=[pltpu.VMEM((width_a * group, LANES), jnp.float32)],
    )(total, amplitudes, energy_a[:, None, None], energy_b[None, :, None], energy_c[None, None, :])


def by_slabs(sizes, amplitudes, factors, energies):
    width_a, width_b, width_c = amplitudes.shape
    fitting, size, _ = factors.shape
    n_a, n_b, n_c = sizes
    peers = n_a * n_c
    share = width_b // peers
    rows = width_a * width_c // LANES
    stacked = factors.reshape(fitting * size, size)
    closing = factors.transpose(0, 2, 1).reshape(fitting * size, size)
    energy_a = lax.dynamic_slice_in_dim(energies, lax.axis_index("aa") * width_a, width_a, 0)
    energy_b = lax.dynamic_slice_in_dim(energies, lax.axis_index("ba") * width_b, width_b, 0)
    energy_c = lax.dynamic_slice_in_dim(energies, lax.axis_index("col") * width_c, width_c, 0)
    packed = pack(amplitudes, 16, rows).reshape(peers, share * rows, LANES)
    portion = lax.all_to_all(packed, ("aa", "col"), 0, 0, tiled=True).reshape(peers, share, rows, LANES)
    ladder, crossing = ladders_of_slabs((n_a, n_c, width_a, width_c, share), portion, stacked, closing, 4)
    crossing = crossing.reshape(n_b, n_a, n_c, share * share, size).transpose(1, 0, 2, 3, 4)
    crossing = crossing.reshape(n_a * n_b * n_c, share * share, size)
    crossing = lax.all_to_all(crossing, ("aa", "ba", "col"), 0, 0, tiled=True)
    total = joined((n_a, n_b, n_c, width_a, width_c, rows), ladder, crossing)
    total = lax.all_to_all(total.reshape(peers, share * rows, LANES), ("aa", "col"), 0, 0, tiled=True)
    return closed(total.reshape(width_b, rows, LANES), amplitudes, energy_a, energy_b, energy_c, 16)


def fits(sizes, shape, size):
    n_a, n_b, n_c = sizes
    width_a, width_b, width_c = shape
    spare = LANES - width_c
    if spare <= 0 or width_c % spare or width_a * width_c % LANES or size % LANES:
        return False
    rows = width_a * width_c // LANES
    share = width_b // (n_a * n_c)
    return (
        rows % 16 == 0
        and (width_a - rows) * (width_c // spare) == rows
        and width_b % (n_a * n_c) == 0
        and share % 4 == 0
        and width_b % 16 == 0
    )


def solution(mesh):
    sizes = tuple(mesh.shape[name] for name in ("aa", "ba", "col"))

    def body(amplitudes, factors, energies):
        if fits(sizes, amplitudes.shape, factors.shape[1]):
            return by_slabs(sizes, amplitudes, factors, energies)
        return on_device(amplitudes, factors, energies)

    return jax.shard_map(
        body,
        mesh=mesh,
        in_specs=(P("aa", "ba", "col"), P(), P()),
        out_specs=P("aa", "ba", "col"),
        check_vma=False,
    )
```
